32 devices in a mesh: rep: 2 (over x), model: 4 (over z), vocab: 4 (over y, core).
Axes of the slice: x: 2, y: 2, z: 4, core: 2. Of those that a mesh axis runs over, the one named last changes fastest.
Arguments:
- hidden: bfloat16 [1024, 3072], P(('rep', 'model', 'vocab')), parts along dimension 0
- head_rows: bfloat16 [128256, 3072], P(('model', 'vocab'))
- allowed_ids: int32 [1024, 64], P(('rep', 'model', 'vocab')), parts along dimension 0
- valid_mask: int32 [1024, 64], P(('rep', 'model', 'vocab')), parts along dimension 0
- target_pos: int32 [1024], P(('rep', 'model', 'vocab')), parts along dimension 0
Outputs:
- output 1: float32 [1024, 64], P(('rep', 'model', 'vocab')), parts along dimension 0
- output 2: float32 [1024], P(('rep', 'model', 'vocab')), parts along dimension 0
There are 2 independent parts. The reference program is written for one: setup_inputs(seed, part) draws one part's arguments, and reference() takes and returns one part's arrays. A program takes and returns all parts, laid end to end along the dimension named above; an argument that names none is the same for every part.
All inputs are finite; a program needn't handle non-finite values.
Results may differ from the reference program's by a relative error of at most 0.001.
Values are sent between devices in bfloat16 or wider.
A program may use at most 1 GiB of HBM per device.

```python
import jax
import jax.numpy as jnp
from jax import lax

VOCAB_SIZE = 128256
MODEL_WIDTH = 3072
NUM_ROWS = 512
LIST_LEN = 64
NUM_SHARDS = 16
OWNER_RUNS = 4
TEMPERATURE = 0.5


def draw_lists(idx_key):
    shard_len = VOCAB_SIZE // NUM_SHARDS
    run_len = LIST_LEN // OWNER_RUNS
    key_rot, key_step, key_start, key_count, key_target = jax.random.split(idx_key, 5)
    rotation = jax.random.randint(key_rot, (NUM_ROWS, 1), 0, NUM_SHARDS - 1)
    run_index = jnp.arange(OWNER_RUNS)[None, :]
    owners = jnp.where(run_index == 0, 0, 1 + (rotation + run_index - 1) % (NUM_SHARDS - 1))
    stride = jax.random.randint(key_step, (NUM_ROWS, OWNER_RUNS), 1, shard_len // run_len + 1)
    run_start = jax.random.randint(key_start, (NUM_ROWS, OWNER_RUNS), 0, shard_len - stride * (run_len - 1))
    offsets = run_start[:, :, None] + stride[:, :, None] * jnp.arange(run_len)[None, None, :]
    allowed_ids = (owners[:, :, None] * shard_len + offsets).reshape(NUM_ROWS, LIST_LEN).astype(jnp.int32)
    counts = LIST_LEN - jax.random.randint(key_count, (NUM_ROWS,), 0, LIST_LEN // 2)
    counts = jnp.where(jnp.arange(NUM_ROWS) == 0, LIST_LEN, counts)
    valid_mask = (jnp.arange(LIST_LEN)[None, :] < counts[:, None]).astype(jnp.int32)
    target_pos = jax.random.randint(key_target, (NUM_ROWS,), 0, counts).astype(jnp.int32)
    return allowed_ids, valid_mask, target_pos


def setup_inputs(seed: int = 0, part: int = 0) -> dict:
    base_key = jax.random.key(seed)
    part_key = jax.random.fold_in(base_key, part)
    key_hidden, key_lists = jax.random.split(part_key, 2)
    hidden = jax.random.normal(key_hidden, (NUM_ROWS, MODEL_WIDTH), jnp.float32).astype(jnp.bfloat16)
    head_rows = (jax.random.normal(jax.random.key(seed + 1), (VOCAB_SIZE, MODEL_WIDTH), jnp.float32) * MODEL_WIDTH ** -0.5).astype(jnp.bfloat16)
    allowed_ids, valid_mask, target_pos = draw_lists(key_lists)
    return {'hidden': hidden, 'head_rows': head_rows, 'allowed_ids': allowed_ids, 'valid_mask': valid_mask, 'target_pos': target_pos}


def reference(hidden, head_rows, allowed_ids, valid_mask, target_pos):
    def row_scores(row_args):
        h_row, row_ids = row_args
        return jnp.dot(head_rows[row_ids], h_row, preferred_element_type=jnp.float32)

    scores = lax.map(row_scores, (hidden, allowed_ids)) / TEMPERATURE
    is_valid = valid_mask > 0
    scores = jnp.where(is_valid, scores, -jnp.inf)
    top_score = jnp.max(scores, axis=1, keepdims=True)
    log_norm = top_score[:, 0] + jnp.log(jnp.sum(jnp.exp(scores - top_score), axis=1))
    probs = jnp.where(is_valid, jnp.exp(scores - log_norm[:, None]), 0.0)
    picked_score = jnp.take_along_axis(scores, target_pos[:, None], axis=1)[:, 0]
    return probs, picked_score - log_norm
```

```python
import functools

import jax
import jax.numpy as jnp
from jax import lax
from jax.experimental import pallas as pl
from jax.experimental.pallas import tpu as pltpu
from jax.sharding import PartitionSpec as P

TEMPERATURE = 0.5
MESH = pl.DeviceIdType.MESH
PAIR = 512
NPAIR = 4
LANES = 128
HALVES = 2


def head_kernel(h_hbm, w_hbm, ids_hbm, ids_ref, valid_ref, tgt_ref, p_ref, lp_ref,
                w, h, ids_all, lane, tile, picks, back, sbuf0, sbuf1,
                w_sem, own_sem, own_ids_sem, h_recv, ids_recv, send_sem, back_send, back_recv):
    m = lax.axis_index('model')
    v = lax.axis_index('vocab')
    c = lax.rem(v, 2)
    y = v // 2
    me = m * 4 + v
    loc, width = h_hbm.shape
    shard_len = w_hbm.shape[0]
    list_len = ids_hbm.shape[1]
    half_w = width // HALVES
    rows_half = 8 * loc
    zbase = (m // 2) * 2
    zp = m + 1 - 2 * lax.rem(m, 2)
    far_near = jnp.where(m < 2, 2, 1)
    far_far = jnp.where(m < 2, 3, 0)
    v_sib = v + 1 - 2 * c
    v_y = lax.rem(v + 2, 4)
    dev_y = {'vocab': v_y}
    dev_zp = {'model': zp}
    dev_sib = {'vocab': v_sib}
    dev_fn = {'model': far_near}
    dev_ff = {'model': far_far}

    def w_copy(i):
        n_rows = min(PAIR, shard_len - i * PAIR)
        return pltpu.make_async_copy(w_hbm.at[pl.ds(i * PAIR, n_rows)], w.at[pl.ds(i * PAIR, n_rows)], w_sem.at[i])

    n_w = pl.cdiv(shard_len, PAIR)

    def h_unit(blk, half):
        return h.at[pl.ds(pl.multiple_of(blk * loc, loc), loc), pl.ds(half * half_w, half_w)]

    def ids_unit(blk):
        return ids_all.at[pl.ds(pl.multiple_of(blk * loc, loc), loc)]

    own_h = pltpu.make_async_copy(h_hbm, h.at[pl.ds(pl.multiple_of(me * loc, loc), loc)], own_sem)
    own_h.start()
    own_ids = pltpu.make_async_copy(ids_hbm, ids_unit(me), own_ids_sem)
    own_ids.start()
    for i in range(n_w):
        w_copy(i).start()

    barrier = pltpu.get_barrier_semaphore()
    peers = (dev_y, dev_zp, dev_sib, dev_fn, dev_ff)
    for d in peers:
        pl.semaphore_signal(barrier, inc=1, device_id=d, device_id_type=MESH)

    pending = []

    def h_copy(k, blk, half, dev):
        return pltpu.make_async_remote_copy(h_unit(blk, half), h_unit(blk, half), send_sem.at[k], h_recv.at[blk, half],
                                            device_id=dev, device_id_type=MESH)

    def ids_copy(k, blk, dev):
        return pltpu.make_async_remote_copy(ids_unit(blk), ids_unit(blk), send_sem.at[k], ids_recv.at[blk],
                                            device_id=dev, device_id_type=MESH)

    def send_h(blk, half, dev):
        h_copy(len(pending), blk, half, dev).start()
        pending.append(functools.partial(h_copy, len(pending), blk, half, dev))

    def send_ids(blk, dev):
        ids_copy(len(pending), blk, dev).start()
        pending.append(functools.partial(ids_copy, len(pending), blk, dev))

    def wait_h(blk, half):
        pltpu.make_async_remote_copy(h_unit(blk, half), h_unit(blk, half), send_sem.at[0], h_recv.at[blk, half],
                                     device_id=dev_sib, device_id_type=MESH).wait_recv()

    def wait_ids(blk):
        pltpu.make_async_remote_copy(ids_unit(blk), ids_unit(blk), send_sem.at[0], ids_recv.at[blk],
                                     device_id=dev_sib, device_id_type=MESH).wait_recv()

    def blk(zz, vv):
        return zz * 4 + vv

    b_y, b_z, b_d = blk(m, v_y), blk(zp, v), blk(zp, v_y)
    s_own, s_y, s_z, s_d = blk(m, v_sib), blk(m, lax.rem(v_sib + 2, 4)), blk(zp, v_sib), blk(zp, lax.rem(v_sib + 2, 4))
    b_fn, b_ff, b_fny, b_ffy = blk(far_near, v), blk(far_far, v), blk(far_near, v_y), blk(far_far, v_y)
    s_fn, s_ff = blk(far_near, v_sib), blk(far_far, v_sib)
    s_fny, s_ffy = blk(far_near, lax.rem(v_sib + 2, 4)), blk(far_far, lax.rem(v_sib + 2, 4))

    own_h.wait()
    own_ids.wait()
    pl.semaphore_wait(barrier, len(peers))

    send_h(me, 0, dev_y)
    send_h(me, 1, dev_zp)
    send_h(me, 1, dev_y)
    send_h(me, 0, dev_zp)
    send_h(me, 0, dev_sib)
    send_h(me, 1, dev_sib)
    for d in (dev_y, dev_zp, dev_sib):
        send_ids(me, d)

    wait_h(b_y, 0)
    send_h(b_y, 0, dev_zp)
    wait_h(b_z, 1)
    send_h(b_z, 1, dev_y)
    for d in (dev_fn, dev_ff):
        send_h(me, 0, d)
        send_h(me, 1, d)
        send_ids(me, d)
    send_h(b_y, 0, dev_sib)
    send_h(b_z, 1, dev_sib)
    wait_ids(b_y)
    send_ids(b_y, dev_zp)
    send_ids(b_y, dev_sib)
    wait_ids(b_z)
    send_ids(b_z, dev_sib)
    wait_h(b_y, 1)
    send_h(b_y, 1, dev_sib)
    wait_h(b_z, 0)
    send_h(b_z, 0, dev_sib)
    wait_ids(b_d)
    send_ids(b_d, dev_sib)
    for half in range(HALVES):
        wait_h(b_d, half)
        send_h(b_d, half, dev_sib)

    def far_first(b, half):
        wait_h(b, half)
        send_h(b, half, dev_y)
        send_h(b, half, dev_sib)

    def far_ids(b):
        wait_ids(b)
        send_ids(b, dev_y)
        send_ids(b, dev_sib)

    def far_second(b, half):
        wait_h(b, half)
        send_h(b, half, dev_sib)

    def point_0():
        pass

    def point_1():
        far_ids(b_fn)
        far_first(b_fn, 0)
        far_first(b_fn, 1)

    def point_2():
        wait_ids(b_fny)
        send_ids(b_fny, dev_sib)
        far_second(b_fny, 0)
        far_second(b_fny, 1)
        far_ids(b_ff)
        far_first(b_ff, 0)

    def point_3():
        far_first(b_ff, 1)

    def final_far():
        wait_ids(b_ffy)
        send_ids(b_ffy, dev_sib)
        far_second(b_ffy, 0)
        far_second(b_ffy, 1)
        for b in (s_fn, s_fny, s_ff, s_ffy):
            wait_ids(b)
            wait_h(b, 0)
            wait_h(b, 1)

    picks[...] = jnp.zeros_like(picks)

    def set_lists(r0):
        off = ids_all[pl.ds(r0, rows_half), :] - me * shard_len
        off = jnp.concatenate([off, off], axis=1)
        lane[...] = jnp.bitwise_and(off, LANES - 1)
        good = jnp.logical_and(off >= 0, off < shard_len)
        tile[...] = jnp.where(good, lax.shift_right_arithmetic(off, 7), 1 << 20)

    sbufs = (sbuf0, sbuf1)
    n_steps = w.shape[0] // (PAIR * NPAIR)

    def run_phase(r0, points):
        hr = pl.ds(r0, rows_half)

        def pick(s_ref, t0):
            for q in range(PAIR // LANES):
                g = jnp.take_along_axis(s_ref[:, q * LANES:(q + 1) * LANES], lane[...], axis=1)
                picks[hr, :] = jnp.where(tile[...] == t0 + q, g, picks[hr, :])

        def step(n, carry):
            for k, point in enumerate(points):
                if point is not None:
                    pl.when(n == k)(point)
            for j in range(NPAIR):
                rows = pl.ds(pl.multiple_of((n * NPAIR + j) * PAIR, PAIR), PAIR)
                sbufs[j % 2][...] = lax.dot_general(h[hr, :], w[rows, :], (((1,), (1,)), ((), ())),
                                                    preferred_element_type=jnp.float32)
                pick(sbufs[(j + 1) % 2], (n * NPAIR + j - 1) * (PAIR // LANES))
            return carry

        lax.fori_loop(0, n_steps, step, 0)
        pick(sbufs[(NPAIR - 1) % 2], (n_steps * NPAIR - 1) * (PAIR // LANES))

    def with_w(k, point):
        def run():
            for i in range(k * NPAIR, min((k + 1) * NPAIR, n_w)):
                w_copy(i).wait()
            point()
        return run

    def send_back(zz, vv, i):
        b = blk(zz, vv)
        cp = pltpu.make_async_remote_copy(picks.at[pl.ds(pl.multiple_of(b * loc, loc), loc)], back.at[me], back_send.at[i],
                                          back_recv.at[me], device_id={'model': zz, 'vocab': vv}, device_id_type=MESH)
        cp.start()
        return cp

    for b in (s_own, s_y, s_z, s_d):
        wait_ids(b)
        wait_h(b, 0)
        wait_h(b, 1)
    r_a = pl.multiple_of((m // 2) * rows_half, rows_half)
    r_b = pl.multiple_of((1 - m // 2) * rows_half, rows_half)
    set_lists(r_a)
    run_phase(r_a, [with_w(k, p) for k, p in enumerate((point_0, point_1, point_2, point_3))])
    backs = []
    for i, (zz, dv) in enumerate([(m, 1), (m, 2), (m, 3), (zp, 0), (zp, 1), (zp, 2), (zp, 3)]):
        backs.append(send_back(zz, lax.rem(v + dv, 4), i))
    final_far()
    set_lists(r_b)
    run_phase(r_b, [])
    for i, (zz, dv) in enumerate([(far_ff, dv) for far_ff in (far_far, far_near) for dv in range(4)]):
        backs.append(send_back(zz, lax.rem(v + dv, 4), 7 + i))

    back[me] = picks[pl.ds(pl.multiple_of(me * loc, loc), loc), :]
    total = back[me]
    for dz in range(4):
        for dv in range(4):
            if dz == 0 and dv == 0:
                continue
            b = blk(lax.rem(m + dz, 4), lax.rem(v + dv, 4))
            pltpu.make_async_remote_copy(back.at[b], back.at[b], back_send.at[0], back_recv.at[b],
                                         device_id=dev_sib, device_id_type=MESH).wait_recv()
            total = total + back[b]
    is_valid = valid_ref[...] > 0
    scores = jnp.where(is_valid, total[:, :list_len] / TEMPERATURE, -jnp.inf)
    top = jnp.max(scores, axis=1, keepdims=True)
    log_norm = top + jnp.log(jnp.sum(jnp.exp(scores - top), axis=1, keepdims=True))
    p_ref[...] = jnp.where(is_valid, jnp.exp(scores - log_norm), 0.0)
    eye = lax.broadcasted_iota(jnp.int32, (loc, loc), 0) == lax.broadcasted_iota(jnp.int32, (loc, loc), 1)
    tgt_col = jnp.sum(jnp.where(eye, tgt_ref[...], 0), axis=1, keepdims=True)
    hit = lax.broadcasted_iota(jnp.int32, (loc, list_len), 1) == tgt_col
    picked = jnp.sum(jnp.where(hit, scores, 0.0), axis=1, keepdims=True)
    lp_ref[...] = jnp.sum(jnp.where(eye, picked - log_norm, 0.0), axis=0, keepdims=True)
    for make in pending:
        make().wait_send()
    for cp in backs:
        cp.wait_send()


def solution(mesh):
    axes = ('model', 'vocab')
    row_spec = P(('rep',) + axes, None)
    vec_spec = P(('rep',) + axes)

    def local_step(hidden, head_rows, allowed_ids, valid_mask, target_pos):
        loc, width = hidden.shape
        list_len = allowed_ids.shape[1]
        rows = 16 * loc
        block = PAIR * NPAIR
        w_rows = pl.cdiv(head_rows.shape[0], block) * block
        any_spec = pl.BlockSpec(memory_space=pl.ANY)
        vmem = pl.BlockSpec(memory_space=pltpu.VMEM)
        dma = pltpu.SemaphoreType.DMA
        p, lp = pl.pallas_call(
            head_kernel,
            out_shape=(jax.ShapeDtypeStruct((loc, list_len), jnp.float32), jax.ShapeDtypeStruct((1, loc), jnp.float32)),
            in_specs=[any_spec, any_spec, any_spec, vmem, vmem, vmem],
            out_specs=(vmem, vmem),
            scratch_shapes=[
                pltpu.VMEM((w_rows, width), jnp.bfloat16),
                pltpu.VMEM((rows, width), jnp.bfloat16),
                pltpu.VMEM((rows, list_len), jnp.int32),
                pltpu.VMEM((rows // 2, LANES), jnp.int32),
                pltpu.VMEM((rows // 2, LANES), jnp.int32),
                pltpu.VMEM((rows, LANES), jnp.float32),
                pltpu.VMEM((16, loc, LANES), jnp.float32),
                pltpu.VMEM((rows // 2, PAIR), jnp.float32),
                pltpu.VMEM((rows // 2, PAIR), jnp.float32),
                dma((pl.cdiv(head_rows.shape[0], PAIR),)),
                dma, dma,
                dma((16, HALVES)),
                dma((16,)),
                dma((64,)),
                dma((16,)),
                dma((16,)),
            ],
            compiler_params=pltpu.CompilerParams(collective_id=0, has_side_effects=True, vmem_limit_bytes=67043328),
        )(hidden, head_rows, allowed_ids, allowed_ids, valid_mask, target_pos.reshape(1, loc))
        return p, lp.reshape(loc)

    return jax.shard_map(local_step, mesh=mesh, in_specs=(row_spec, P(axes, None), row_spec, row_spec, vec_spec),
                         out_specs=(row_spec, vec_spec), check_vma=False)
```

```python
import functools

import jax
import jax.numpy as jnp
from jax import lax
from jax.experimental import pallas as pl
from jax.experimental.pallas import tpu as pltpu
from jax.sharding import PartitionSpec as P

TEMPERATURE = 0.5
MESH = pl.DeviceIdType.MESH
PAIR = 512
NPAIR = 4
LANES = 128
W_ROWS = 1024
CHUNKS_PER_STEP = PAIR * NPAIR // W_ROWS
ALL, INNER, OUTER = 0, 1, 2


def head_kernel(h_hbm, w_hbm, ids_hbm, valid_ref, tgt_ref, p_ref, lp_ref,
                w, h, acc, ids_all, lane, tile, picks, packed, back, sbuf0, sbuf1,
                w_sem, own_sem, own_ids_sem, h_recv, ids_recv, send_sem, back_send, back_recv):
    m = lax.axis_index('model')
    v = lax.axis_index('vocab')
    c = lax.rem(v, 2)
    me = m * 4 + v
    loc, width = h_hbm.shape
    shard_len = w_hbm.shape[0]
    list_len = ids_hbm.shape[1]
    quarter = width // 4
    half_w = width // 2
    rows_half = 8 * loc
    zp = m + 1 - 2 * lax.rem(m, 2)
    inner_n = m * (3 - m) // 2
    inner = inner_n == 1
    far_near = jnp.where(m < 2, 2, 1)
    far_far = jnp.where(m < 2, 3, 0)
    v_sib = v + 1 - 2 * c
    v_y = lax.rem(v + 2, 4)
    v_sy = lax.rem(v_sib + 2, 4)
    dev_y = {'vocab': v_y}
    dev_zp = {'model': zp}
    dev_sib = {'vocab': v_sib}
    dev_across = {'model': jnp.where(m < 2, 2, 1)}
    near_peers = (dev_y, dev_zp, dev_sib)

    n_chunks = pl.cdiv(shard_len, W_ROWS)

    def w_copy(i, half):
        n_rows = min(W_ROWS, shard_len - i * W_ROWS)
        at = (pl.ds(i * W_ROWS, n_rows), pl.ds(half * half_w, half_w))
        return pltpu.make_async_copy(w_hbm.at[at], w.at[at], w_sem.at[i, half])

    def row_block(blk):
        return pl.ds(pl.multiple_of(blk * loc, loc), loc)

    own_h = pltpu.make_async_copy(h_hbm, h.at[row_block(me)], own_sem)
    own_h.start()
    own_ids = pltpu.make_async_copy(ids_hbm, ids_all.at[row_block(me)], own_ids_sem)
    own_ids.start()
    barrier = pltpu.get_barrier_semaphore()
    for d in near_peers:
        pl.semaphore_signal(barrier, inc=1, device_id=d, device_id_type=MESH)

    @pl.when(inner)
    def _():
        pl.semaphore_signal(barrier, inc=1, device_id=dev_across, device_id_type=MESH)

    for half in range(2):
        for i in range(n_chunks):
            w_copy(i, half).start(priority=1)

    sent = {ALL: [], INNER: []}
    n_sent = [0]

    def h_copy(k, blk, piece, dev):
        ref = h.at[row_block(blk), pl.ds(piece[0] * quarter, piece[1] * quarter)]
        return pltpu.make_async_remote_copy(ref, ref, send_sem.at[k], h_recv.at[blk, piece[0]],
                                            device_id=dev, device_id_type=MESH)

    def ids_copy(k, blk, dev):
        ref = ids_all.at[row_block(blk)]
        return pltpu.make_async_remote_copy(ref, ref, send_sem.at[k], ids_recv.at[blk],
                                            device_id=dev, device_id_type=MESH)

    def start(make, who):
        make(n_sent[0]).start()
        sent[who].append(functools.partial(make, n_sent[0]))
        n_sent[0] += 1

    def send_h(blk, piece, dev, who=0):
        start(lambda k: h_copy(k, blk, piece, dev), who)

    def send_ids(blk, dev, who=0):
        start(lambda k: ids_copy(k, blk, dev), who)

    def wait_h(blk, piece):
        h_copy(0, blk, piece, dev_sib).wait_recv()

    def wait_ids(blk):
        ids_copy(0, blk, dev_sib).wait_recv()

    def blk(zz, vv):
        return zz * 4 + vv

    b_y, b_z, b_d = blk(m, v_y), blk(zp, v), blk(zp, v_y)
    near_sib = (blk(m, v_sib), blk(m, v_sy), blk(zp, v_sib), blk(zp, v_sy))
    b_fn, b_ff, b_fny, b_ffy = blk(far_near, v), blk(far_far, v), blk(far_near, v_y), blk(far_far, v_y)
    far_sib = (blk(far_near, v_sib), blk(far_far, v_sib), blk(far_near, v_sy), blk(far_far, v_sy))
    quarters = tuple((q, 1) for q in range(4))
    halves = ((0, 2), (2, 2))

    own_h.wait()
    own_ids.wait()
    pl.semaphore_wait(barrier, 3 + inner_n)

    send_h(me, quarters[0], dev_y)
    send_h(me, quarters[1], dev_zp)
    send_h(me, quarters[1], dev_y)
    send_h(me, quarters[0], dev_zp)

    @pl.when(inner)
    def _():
        send_h(me, halves[0], dev_across, INNER)

    send_h(me, halves[0], dev_sib)
    wait_h(b_y, quarters[0])
    send_h(b_y, quarters[0], dev_zp)
    wait_h(b_z, quarters[1])
    send_h(b_z, quarters[1], dev_y)
    send_h(me, quarters[2], dev_y)
    send_h(me, quarters[3], dev_zp)
    send_h(me, quarters[3], dev_y)
    send_h(me, quarters[2], dev_zp)
    send_h(me, halves[1], dev_sib)
    for d in near_peers:
        send_ids(me, d)
    wait_h(b_y, quarters[1])
    send_h(b_y, halves[0], dev_sib)
    wait_h(b_z, quarters[0])
    send_h(b_z, halves[0], dev_sib)

    @pl.when(inner)
    def _():
        send_h(b_z, halves[0], dev_across, INNER)
        send_h(me, halves[1], dev_across, INNER)
        send_ids(me, dev_across, INNER)

    def far(b, half):
        wait_h(b, halves[half])
        send_h(b, halves[half], dev_y, INNER)
        send_h(b, halves[half], dev_zp, INNER)
        send_h(b, halves[half], dev_sib, INNER)
        if half:
            wait_ids(b)
            for d in (dev_y, dev_zp, dev_sib):
                send_ids(b, d, INNER)

    def far_outer(b, half):
        wait_h(b, halves[half])
        send_h(b, halves[half], dev_y, OUTER)
        send_h(b, halves[half], dev_sib, OUTER)
        if half:
            wait_ids(b)
            for d in (dev_y, dev_sib):
                send_ids(b, d, OUTER)

    def far_y(b, half, who):
        wait_h(b, halves[half])
        send_h(b, halves[half], dev_sib, who)
        if half:
            wait_ids(b)
            send_ids(b, dev_sib, who)

    sent[OUTER] = []
    outer = inner_n == 0

    pl.when(inner)(lambda: far(b_fn, 0))
    wait_h(b_d, quarters[0])
    wait_h(b_d, quarters[1])
    send_h(b_d, halves[0], dev_sib)
    for b in near_sib:
        wait_h(b, halves[0])

    def wait_w(i, half):
        for k in range(CHUNKS_PER_STEP):
            if i * CHUNKS_PER_STEP + k < n_chunks:
                w_copy(i * CHUNKS_PER_STEP + k, half).wait()

    def a0_0():
        wait_w(0, 0)

    def a0_1():
        wait_w(1, 0)
        wait_h(b_y, quarters[2])
        send_h(b_y, quarters[2], dev_zp)
        wait_h(b_z, quarters[3])
        send_h(b_z, quarters[3], dev_y)
        wait_h(b_y, quarters[3])
        send_h(b_y, halves[1], dev_sib)
        wait_h(b_z, quarters[2])
        send_h(b_z, halves[1], dev_sib)
        wait_ids(b_y)
        send_ids(b_y, dev_zp)
        send_ids(b_y, dev_sib)
        wait_ids(b_z)
        send_ids(b_z, dev_sib)

        @pl.when(inner)
        def _():
            send_h(b_z, halves[1], dev_across, INNER)
            send_ids(b_z, dev_across, INNER)
            far(b_ff, 0)

    def a0_2():
        wait_w(2, 0)

        @pl.when(inner)
        def _():
            far(b_fn, 1)
            far_y(b_fny, 0, INNER)

        pl.when(outer)(lambda: far_outer(b_fn, 0))

    def a0_3():
        wait_w(3, 0)
        wait_h(b_d, quarters[2])
        wait_h(b_d, quarters[3])
        send_h(b_d, halves[1], dev_sib)
        wait_ids(b_d)
        send_ids(b_d, dev_sib)

    def a1_0():
        wait_w(0, 1)

        @pl.when(inner)
        def _():
            far(b_ff, 1)
            far_y(b_ffy, 0, INNER)

        pl.when(outer)(lambda: far_outer(b_ff, 0))

    def a1_1():
        wait_w(1, 1)
        pl.when(outer)(lambda: far_y(b_fny, 0, OUTER))

    def a1_2():
        wait_w(2, 1)
        pl.when(inner)(lambda: far_y(b_fny, 1, INNER))
        pl.when(outer)(lambda: far_outer(b_fn, 1))

    def a1_3():
        wait_w(3, 1)
        pl.when(inner)(lambda: far_y(b_ffy, 1, INNER))

        @pl.when(outer)
        def _():
            far_outer(b_ff, 1)
            far_y(b_ffy, 0, OUTER)

    def b0_1():
        pl.when(outer)(lambda: far_y(b_fny, 1, OUTER))

    def b0_2():
        pl.when(outer)(lambda: far_y(b_ffy, 1, OUTER))

    picks[...] = jnp.zeros_like(picks)

    def set_lists(r0):
        off = ids_all[pl.ds(r0, rows_half), :] - me * shard_len
        off = jnp.concatenate([off, off], axis=1)
        lane[...] = jnp.bitwise_and(off, LANES - 1)
        good = jnp.logical_and(off >= 0, off < shard_len)
        tile[...] = jnp.where(good, lax.shift_right_arithmetic(off, 7), 1 << 20)

    sbufs = (sbuf0, sbuf1)
    n_steps = w.shape[0] // (PAIR * NPAIR)

    def run_phase(r0, half, points):
        hr = pl.ds(r0, rows_half)
        kc = pl.ds(half * half_w, half_w)

        def pick(s_ref, t0):
            for q in range(PAIR // LANES):
                g = jnp.take_along_axis(s_ref[:, q * LANES:(q + 1) * LANES], lane[...], axis=1)
                picks[hr, :] = jnp.where(tile[...] == t0 + q, g, picks[hr, :])

        def step(n, carry):
            for k, point in enumerate(points):
                if point is not None:
                    pl.when(n == k)(point)
            for j in range(NPAIR):
                rows = pl.ds(pl.multiple_of((n * NPAIR + j) * PAIR, PAIR), PAIR)
                prod = lax.dot_general(h[hr, kc], w[rows, kc], (((1,), (1,)), ((), ())),
                                       preferred_element_type=jnp.float32)
                if half == 0:
                    acc[n * NPAIR + j] = prod
                else:
                    sbufs[j % 2][...] = prod + acc[n * NPAIR + j]
                    pick(sbufs[(j + 1) % 2], (n * NPAIR + j - 1) * (PAIR // LANES))
            return carry

        lax.fori_loop(0, n_steps, step, 0)
        if half:
            pick(sbufs[(NPAIR - 1) % 2], (n_steps * NPAIR - 1) * (PAIR // LANES))

    low = lax.broadcasted_iota(jnp.int32, (loc // 2, LANES), 1) < list_len

    def pack(r0, p0):
        for i in range(8):
            top = picks[pl.ds(pl.multiple_of(r0 + i * loc, loc // 2), loc // 2), :]
            bot = picks[pl.ds(pl.multiple_of(r0 + i * loc + loc // 2, loc // 2), loc // 2), :]
            packed[p0 + i] = jnp.where(low, top, bot)

    def send_back(zz, vv, i):
        cp = pltpu.make_async_remote_copy(packed.at[blk(zz, vv)], back.at[me], back_send.at[i], back_recv.at[me],
                                          device_id={'model': zz, 'vocab': vv}, device_id_type=MESH)
        cp.start()
        return cp

    r_a = pl.multiple_of((m // 2) * rows_half, rows_half)
    r_b = pl.multiple_of((1 - m // 2) * rows_half, rows_half)
    run_phase(r_a, 0, (a0_0, a0_1, a0_2, a0_3))
    for b in near_sib:
        wait_ids(b)
        wait_h(b, halves[1])
    set_lists(r_a)
    run_phase(r_a, 1, (a1_0, a1_1, a1_2, a1_3))
    pack(r_a, (m // 2) * 8)
    backs = []
    for i, (zz, dv) in enumerate([(zp, 2), (zp, 3), (zp, 0), (zp, 1), (m, 2), (m, 1), (m, 3)]):
        backs.append(send_back(zz, lax.rem(v + dv, 4), i))
    for b in far_sib:
        wait_h(b, halves[0])
    run_phase(r_b, 0, (None, b0_1, b0_2))
    for b in far_sib:
        wait_ids(b)
        wait_h(b, halves[1])
    set_lists(r_b)
    run_phase(r_b, 1, ())
    pack(r_b, (1 - m // 2) * 8)
    for i, (zz, dv) in enumerate([(zf, dv) for zf in (far_far, far_near) for dv in (2, 3, 0, 1)]):
        backs.append(send_back(zz, lax.rem(v + dv, 4), 7 + i))

    back[me] = packed[me]
    total = back[me]
    for dz in range(4):
        for dv in range(4):
            if dz == 0 and dv == 0:
                continue
            b = blk(lax.rem(m + dz, 4), lax.rem(v + dv, 4))
            pltpu.make_async_remote_copy(back.at[b], back.at[b], back_send.at[0], back_recv.at[b],
                                         device_id=dev_sib, device_id_type=MESH).wait_recv()
            total = total + back[b]
    total = jnp.concatenate([total, pltpu.roll(total, LANES - list_len, 1)], axis=0)[:, :list_len]
    is_valid = valid_ref[...] > 0
    scores = jnp.where(is_valid, total / TEMPERATURE, -jnp.inf)
    top = jnp.max(scores, axis=1, keepdims=True)
    log_norm = top + jnp.log(jnp.sum(jnp.exp(scores - top), axis=1, keepdims=True))
    p_ref[...] = jnp.where(is_valid, jnp.exp(scores - log_norm), 0.0)
    eye = lax.broadcasted_iota(jnp.int32, (loc, loc), 0) == lax.broadcasted_iota(jnp.int32, (loc, loc), 1)
    tgt_col = jnp.sum(jnp.where(eye, tgt_ref[...], 0), axis=1, keepdims=True)
    hit = lax.broadcasted_iota(jnp.int32, (loc, list_len), 1) == tgt_col
    picked = jnp.sum(jnp.where(hit, scores, 0.0), axis=1, keepdims=True)
    lp_ref[...] = jnp.sum(jnp.where(eye, picked - log_norm, 0.0), axis=0, keepdims=True)
    for make in sent[ALL]:
        make().wait_send()

    @pl.when(inner)
    def _():
        for make in sent[INNER]:
            make().wait_send()

    @pl.when(outer)
    def _():
        for make in sent[OUTER]:
            make().wait_send()

    for cp in backs:
        cp.wait_send()


def solution(mesh):
    axes = ('model', 'vocab')
    row_spec = P(('rep',) + axes, None)
    vec_spec = P(('rep',) + axes)

    def local_step(hidden, head_rows, allowed_ids, valid_mask, target_pos):
        loc, width = hidden.shape
        list_len = allowed_ids.shape[1]
        rows = 16 * loc
        block = PAIR * NPAIR
        w_rows = pl.cdiv(head_rows.shape[0], block) * block
        any_spec = pl.BlockSpec(memory_space=pl.ANY)
        vmem = pl.BlockSpec(memory_space=pltpu.VMEM)
        dma = pltpu.SemaphoreType.DMA
        p, lp = pl.pallas_call(
            head_kernel,
            out_shape=(jax.ShapeDtypeStruct((loc, list_len), jnp.float32), jax.ShapeDtypeStruct((1, loc), jnp.float32)),
            in_specs=[any_spec, any_spec, any_spec, vmem, vmem],
            out_specs=(vmem, vmem),
            scratch_shapes=[
                pltpu.VMEM((w_rows, width), jnp.bfloat16),
                pltpu.VMEM((rows, width), jnp.bfloat16),
                pltpu.VMEM((w_rows // PAIR, rows // 2, PAIR), jnp.float32),
                pltpu.VMEM((rows, list_len), jnp.int32),
                pltpu.VMEM((rows // 2, LANES), jnp.int32),
                pltpu.VMEM((rows // 2, LANES), jnp.int32),
                pltpu.VMEM((rows, LANES), jnp.float32),
                pltpu.VMEM((16, loc // 2, LANES), jnp.float32),
                pltpu.VMEM((16, loc // 2, LANES), jnp.float32),
                pltpu.VMEM((rows // 2, PAIR), jnp.float32),
                pltpu.VMEM((rows // 2, PAIR), jnp.float32),
                dma((pl.cdiv(head_rows.shape[0], W_ROWS), 2)),
                dma, dma,
                dma((16, 4)),
                dma((16,)),
                dma((96,)),
                dma((16,)),
                dma((16,)),
            ],
            compiler_params=pltpu.CompilerParams(collective_id=0, has_side_effects=True, vmem_limit_bytes=67043328),
        )(hidden, head_rows, allowed_ids, valid_mask, target_pos.reshape(1, loc))
        return p, lp.reshape(loc)

    return jax.shard_map(local_step, mesh=mesh, in_specs=(row_spec, P(axes, None), row_spec, row_spec, vec_spec),
                         out_specs=(row_spec, vec_spec), check_vma=False)
```

```python
import functools

import jax
import jax.numpy as jnp
from jax import lax
from jax.experimental import pallas as pl
from jax.experimental.pallas import tpu as pltpu
from jax.sharding import PartitionSpec as P

TEMPERATURE = 0.5
MESH = pl.DeviceIdType.MESH
PAIR = 512
LANES = 128
W_ROWS = 1024
ALL, INNER, OUTER = 0, 1, 2


def head_kernel(h_hbm, w_hbm, ids_hbm, valid_hbm, tgt_hbm, p_ref, lp_ref,
                valid_ref, tgt_ref, w, h, acc, ids_all, lane, tile, picks, packed, back, sbuf0, sbuf1,
                w_sem, own_sem, own_ids_sem, valid_sem, tgt_sem, h_recv, ids_recv, send_sem, back_send, back_recv):
    m = lax.axis_index('model')
    v = lax.axis_index('vocab')
    c = lax.rem(v, 2)
    me = m * 4 + v
    loc, width = h_hbm.shape
    shard_len = w_hbm.shape[0]
    list_len = ids_hbm.shape[1]
    quarter = width // 4
    half_w = width // 2
    rows_half = 8 * loc
    zp = m + 1 - 2 * lax.rem(m, 2)
    inner_n = m * (3 - m) // 2
    inner = inner_n == 1
    far_near = jnp.where(m < 2, 2, 1)
    far_far = jnp.where(m < 2, 3, 0)
    v_sib = v + 1 - 2 * c
    v_y = lax.rem(v + 2, 4)
    v_sy = lax.rem(v_sib + 2, 4)
    dev_y = {'vocab': v_y}
    dev_zp = {'model': zp}
    dev_sib = {'vocab': v_sib}
    dev_across = {'model': jnp.where(m < 2, 2, 1)}
    near_peers = (dev_y, dev_zp, dev_sib)

    n_chunks = pl.cdiv(shard_len, W_ROWS)

    def w_copy(i, half):
        n_rows = min(W_ROWS, shard_len - i * W_ROWS)
        at = (pl.ds(i * W_ROWS, n_rows), pl.ds(half * half_w, half_w))
        return pltpu.make_async_copy(w_hbm.at[at], w.at[at], w_sem.at[i, half])

    def row_block(blk):
        return pl.ds(pl.multiple_of(blk * loc, loc), loc)

    barrier = pltpu.get_barrier_semaphore()
    for d in near_peers:
        pl.semaphore_signal(barrier, inc=1, device_id=d, device_id_type=MESH)

    @pl.when(inner)
    def _():
        pl.semaphore_signal(barrier, inc=1, device_id=dev_across, device_id_type=MESH)

    own_h = pltpu.make_async_copy(h_hbm, h.at[row_block(me)], own_sem)
    own_h.start()
    own_valid = pltpu.make_async_copy(valid_hbm, valid_ref, valid_sem)
    own_tgt = pltpu.make_async_copy(tgt_hbm, tgt_ref, tgt_sem)
    own_ids = pltpu.make_async_copy(ids_hbm, ids_all.at[row_block(me)], own_ids_sem)
    own_ids.start()
    own_valid.start()
    own_tgt.start()
    for half in range(2):
        for i in range(n_chunks):
            w_copy(i, half).start(priority=1)

    sent = {ALL: [], INNER: []}
    n_sent = [0]

    def h_copy(k, blk, piece, dev):
        ref = h.at[row_block(blk), pl.ds(piece[0] * quarter, piece[1] * quarter)]
        return pltpu.make_async_remote_copy(ref, ref, send_sem.at[k], h_recv.at[blk, piece[0]],
                                            device_id=dev, device_id_type=MESH)

    def ids_copy(k, blk, dev):
        ref = ids_all.at[row_block(blk)]
        return pltpu.make_async_remote_copy(ref, ref, send_sem.at[k], ids_recv.at[blk],
                                            device_id=dev, device_id_type=MESH)

    def start(make, who):
        make(n_sent[0]).start()
        sent[who].append(functools.partial(make, n_sent[0]))
        n_sent[0] += 1

    def send_h(blk, piece, dev, who=0):
        start(lambda k: h_copy(k, blk, piece, dev), who)

    def send_ids(blk, dev, who=0):
        start(lambda k: ids_copy(k, blk, dev), who)

    def wait_h(blk, piece):
        h_copy(0, blk, piece, dev_sib).wait_recv()

    def wait_ids(blk):
        ids_copy(0, blk, dev_sib).wait_recv()

    def blk(zz, vv):
        return zz * 4 + vv

    b_y, b_z, b_d = blk(m, v_y), blk(zp, v), blk(zp, v_y)
    near_sib = (blk(m, v_sib), blk(m, v_sy), blk(zp, v_sib), blk(zp, v_sy))
    b_fn, b_ff, b_fny, b_ffy = blk(far_near, v), blk(far_far, v), blk(far_near, v_y), blk(far_far, v_y)
    far_sib = (blk(far_near, v_sib), blk(far_far, v_sib), blk(far_near, v_sy), blk(far_far, v_sy))
    quarters = tuple((q, 1) for q in range(4))
    halves = ((0, 2), (2, 2))

    own_h.wait()
    own_ids.wait()
    pl.semaphore_wait(barrier, 3 + inner_n)

    send_h(me, quarters[0], dev_y)
    send_h(me, quarters[1], dev_zp)
    send_h(me, quarters[1], dev_y)
    send_h(me, quarters[0], dev_zp)

    @pl.when(inner)
    def _():
        send_h(me, halves[0], dev_across, INNER)

    send_h(me, halves[0], dev_sib)
    wait_h(b_y, quarters[0])
    send_h(b_y, quarters[0], dev_zp)
    wait_h(b_z, quarters[1])
    send_h(b_z, quarters[1], dev_y)
    send_h(me, quarters[2], dev_y)
    send_h(me, quarters[3], dev_zp)
    send_h(me, quarters[3], dev_y)
    send_h(me, quarters[2], dev_zp)
    send_h(me, halves[1], dev_sib)
    for d in near_peers:
        send_ids(me, d)
    wait_h(b_y, quarters[1])
    send_h(b_y, halves[0], dev_sib)
    wait_h(b_z, quarters[0])
    send_h(b_z, halves[0], dev_sib)

    @pl.when(inner)
    def _():
        send_h(b_z, halves[0], dev_across, INNER)
        send_h(me, halves[1], dev_across, INNER)
        send_ids(me, dev_across, INNER)

    def far(b, half):
        wait_h(b, halves[half])
        send_h(b, halves[half], dev_y, INNER)
        send_h(b, halves[half], dev_zp, INNER)
        send_h(b, halves[half], dev_sib, INNER)
        if half:
            wait_ids(b)
            for d in (dev_y, dev_zp, dev_sib):
                send_ids(b, d, INNER)

    def far_outer(b, half):
        wait_h(b, halves[half])
        send_h(b, halves[half], dev_y, OUTER)
        send_h(b, halves[half], dev_sib, OUTER)
        if half:
            wait_ids(b)
            for d in (dev_y, dev_sib):
                send_ids(b, d, OUTER)

    def far_y(b, half, who):
        wait_h(b, halves[half])
        send_h(b, halves[half], dev_sib, who)
        if half:
            wait_ids(b)
            send_ids(b, dev_sib, who)

    sent[OUTER] = []
    outer = inner_n == 0

    pl.when(inner)(lambda: far(b_fn, 0))
    wait_h(b_d, quarters[0])
    wait_h(b_d, quarters[1])
    send_h(b_d, halves[0], dev_sib)
    wait_h(b_y, quarters[2])
    send_h(b_y, quarters[2], dev_zp)
    wait_h(b_z, quarters[3])
    send_h(b_z, quarters[3], dev_y)
    for b in near_sib:
        wait_h(b, halves[0])

    def wait_w(half):
        for i in range(n_chunks):
            w_copy(i, half).wait()

    def a0_quarter():
        wait_h(b_y, quarters[3])
        send_h(b_y, halves[1], dev_sib)
        wait_h(b_z, quarters[2])
        send_h(b_z, halves[1], dev_sib)
        wait_ids(b_y)
        send_ids(b_y, dev_zp)
        send_ids(b_y, dev_sib)
        wait_ids(b_z)
        send_ids(b_z, dev_sib)

        @pl.when(inner)
        def _():
            send_h(b_z, halves[1], dev_across, INNER)
            send_ids(b_z, dev_across, INNER)
            far(b_ff, 0)

    def a0_half():
        @pl.when(inner)
        def _():
            far(b_fn, 1)
            far_y(b_fny, 0, INNER)

        pl.when(outer)(lambda: far_outer(b_fn, 0))

    def a0_three():
        wait_h(b_d, quarters[2])
        wait_h(b_d, quarters[3])
        send_h(b_d, halves[1], dev_sib)
        wait_ids(b_d)
        send_ids(b_d, dev_sib)

    def a1_start():
        @pl.when(inner)
        def _():
            far(b_ff, 1)
            far_y(b_ffy, 0, INNER)

        pl.when(outer)(lambda: far_outer(b_ff, 0))

    def a1_quarter():
        pl.when(inner)(lambda: far_y(b_fny, 1, INNER))

        @pl.when(outer)
        def _():
            far_outer(b_fn, 1)
            far_y(b_fny, 0, OUTER)

    def a1_three():
        pl.when(inner)(lambda: far_y(b_ffy, 1, INNER))

        @pl.when(outer)
        def _():
            far_outer(b_ff, 1)
            far_y(b_ffy, 0, OUTER)

    def b0_half():
        @pl.when(outer)
        def _():
            far_y(b_fny, 1, OUTER)
            far_y(b_ffy, 1, OUTER)

    picks[...] = jnp.zeros_like(picks)

    def set_lists(r0):
        off = ids_all[pl.ds(r0, rows_half), :] - me * shard_len
        off = jnp.concatenate([off, off], axis=1)
        lane[...] = jnp.bitwise_and(off, LANES - 1)
        good = jnp.logical_and(off >= 0, off < shard_len)
        tile[...] = jnp.where(good, lax.shift_right_arithmetic(off, 7), 1 << 20)

    sbufs = (sbuf0, sbuf1)
    n_pairs = w.shape[0] // PAIR

    def run_pass(r0, half, points):
        hr = pl.ds(r0, rows_half)
        kc = pl.ds(half * half_w, half_w)

        def pick(s_ref, t0):
            for q in range(PAIR // LANES):
                g = jnp.take_along_axis(s_ref[:, q * LANES:(q + 1) * LANES], lane[...], axis=1)
                picks[hr, :] = jnp.where(tile[...] == t0 + q, g, picks[hr, :])

        for j in range(n_pairs):
            if j in points:
                points[j]()
            prod = lax.dot_general(h[hr, kc], w[pl.ds(j * PAIR, PAIR), kc], (((1,), (1,)), ((), ())),
                                   preferred_element_type=jnp.float32)
            if half == 0:
                acc[j] = prod
            else:
                sbufs[j % 2][...] = prod + acc[j]
                if j:
                    pick(sbufs[(j + 1) % 2], (j - 1) * (PAIR // LANES))
        if half:
            pick(sbufs[(n_pairs - 1) % 2], (n_pairs - 1) * (PAIR // LANES))

    low = lax.broadcasted_iota(jnp.int32, (loc // 2, LANES), 1) < list_len

    def pack(r0, p0):
        for i in range(8):
            top = picks[pl.ds(pl.multiple_of(r0 + i * loc, loc // 2), loc // 2), :]
            bot = picks[pl.ds(pl.multiple_of(r0 + i * loc + loc // 2, loc // 2), loc // 2), :]
            packed[p0 + i] = jnp.where(low, top, bot)

    def send_back(zz, vv, i):
        cp = pltpu.make_async_remote_copy(packed.at[blk(zz, vv)], back.at[me], back_send.at[i], back_recv.at[me],
                                          device_id={'model': zz, 'vocab': vv}, device_id_type=MESH)
        cp.start()
        return cp

    r_a = pl.multiple_of((m // 2) * rows_half, rows_half)
    r_b = pl.multiple_of((1 - m // 2) * rows_half, rows_half)
    own_valid.wait()
    own_tgt.wait()
    wait_w(0)
    run_pass(r_a, 0, {4: a0_quarter, 8: a0_half, 12: a0_three})
    for b in near_sib:
        wait_ids(b)
        wait_h(b, halves[1])
    a1_start()
    set_lists(r_a)
    wait_w(1)
    run_pass(r_a, 1, {4: a1_quarter, 12: a1_three})
    pack(r_a, (m // 2) * 8)
    backs = []
    for i, (zz, dv) in enumerate([(zp, 2), (zp, 3), (zp, 0), (zp, 1), (m, 2), (m, 1), (m, 3)]):
        backs.append(send_back(zz, lax.rem(v + dv, 4), i))
    for b in far_sib:
        wait_h(b, halves[0])
    run_pass(r_b, 0, {8: b0_half})
    for b in far_sib:
        wait_ids(b)
        wait_h(b, halves[1])
    set_lists(r_b)
    run_pass(r_b, 1, {})
    pack(r_b, (1 - m // 2) * 8)
    for i, (zz, dv) in enumerate([(zf, dv) for zf in (far_far, far_near) for dv in (2, 3, 0, 1)]):
        backs.append(send_back(zz, lax.rem(v + dv, 4), 7 + i))

    back[me] = packed[me]
    total = back[me]
    for dz in range(4):
        for dv in range(4):
            if dz == 0 and dv == 0:
                continue
            b = blk(lax.rem(m + dz, 4), lax.rem(v + dv, 4))
            pltpu.make_async_remote_copy(back.at[b], back.at[b], back_send.at[0], back_recv.at[b],
                                         device_id=dev_sib, device_id_type=MESH).wait_recv()
            total = total + back[b]
    total = jnp.concatenate([total, pltpu.roll(total, LANES - list_len, 1)], axis=0)[:, :list_len]
    is_valid = valid_ref[...] > 0
    scores = jnp.where(is_valid, total / TEMPERATURE, -jnp.inf)
    top = jnp.max(scores, axis=1, keepdims=True)
    log_norm = top + jnp.log(jnp.sum(jnp.exp(scores - top), axis=1, keepdims=True))
    p_ref[...] = jnp.where(is_valid, jnp.exp(scores - log_norm), 0.0)
    eye = lax.broadcasted_iota(jnp.int32, (loc, loc), 0) == lax.broadcasted_iota(jnp.int32, (loc, loc), 1)
    tgt_col = jnp.sum(jnp.where(eye, tgt_ref[...], 0), axis=1, keepdims=True)
    hit = lax.broadcasted_iota(jnp.int32, (loc, list_len), 1) == tgt_col
    picked = jnp.sum(jnp.where(hit, scores, 0.0), axis=1, keepdims=True)
    lp_ref[...] = jnp.sum(jnp.where(eye, picked - log_norm, 0.0), axis=0, keepdims=True)
    for make in sent[ALL]:
        make().wait_send()

    @pl.when(inner)
    def _():
        for make in sent[INNER]:
            make().wait_send()

    @pl.when(outer)
    def _():
        for make in sent[OUTER]:
            make().wait_send()

    for cp in backs:
        cp.wait_send()


def solution(mesh):
    axes = ('model', 'vocab')
    row_spec = P(('rep',) + axes, None)
    vec_spec = P(('rep',) + axes)

    def local_step(hidden, head_rows, allowed_ids, valid_mask, target_pos):
        loc, width = hidden.shape
        list_len = allowed_ids.shape[1]
        rows = 16 * loc
        w_rows = pl.cdiv(head_rows.shape[0], PAIR) * PAIR
        any_spec = pl.BlockSpec(memory_space=pl.ANY)
        vmem = pl.BlockSpec(memory_space=pltpu.VMEM)
        dma = pltpu.SemaphoreType.DMA
        p, lp = pl.pallas_call(
            head_kernel,
            out_shape=(pltpu.VMEM((loc, list_len), jnp.float32), pltpu.VMEM((1, loc), jnp.float32)),
            in_specs=[any_spec] * 5,
            out_specs=(vmem, vmem),
            scratch_shapes=[
                pltpu.VMEM((loc, list_len), jnp.int32),
                pltpu.VMEM((1, loc), jnp.int32),
                pltpu.VMEM((w_rows, width), jnp.bfloat16),
                pltpu.VMEM((rows, width), jnp.bfloat16),
                pltpu.VMEM((w_rows // PAIR, rows // 2, PAIR), jnp.float32),
                pltpu.VMEM((rows, list_len), jnp.int32),
                pltpu.VMEM((rows // 2, LANES), jnp.int32),
                pltpu.VMEM((rows // 2, LANES), jnp.int32),
                pltpu.VMEM((rows, LANES), jnp.float32),
                pltpu.VMEM((16, loc // 2, LANES), jnp.float32),
                pltpu.VMEM((16, loc // 2, LANES), jnp.float32),
                pltpu.VMEM((rows // 2, PAIR), jnp.float32),
                pltpu.VMEM((rows // 2, PAIR), jnp.float32),
                dma((pl.cdiv(head_rows.shape[0], W_ROWS), 2)),
                dma, dma, dma, dma,
                dma((16, 4)),
                dma((16,)),
                dma((96,)),
                dma((16,)),
                dma((16,)),
            ],
            compiler_params=pltpu.CompilerParams(collective_id=0, has_side_effects=True, vmem_limit_bytes=65500000),
        )(hidden, head_rows, allowed_ids, valid_mask, target_pos.reshape(1, loc))
        return p, lp.reshape(loc)

    return jax.shard_map(local_step, mesh=mesh, in_specs=(row_spec, P(axes, None), row_spec, row_spec, vec_spec),
                         out_specs=(row_spec, vec_spec), check_vma=False)
```

```python
import functools

import jax
import jax.numpy as jnp
from jax import lax
from jax.experimental import pallas as pl
from jax.experimental.pallas import tpu as pltpu
from jax.sharding import PartitionSpec as P

TEMPERATURE = 0.5
MESH = pl.DeviceIdType.MESH
PAIR = 512
LANES = 128
W_ROWS = 1024
ALL, INNER, OUTER = 0, 1, 2
N_SENDS = 57


def head_kernel(h_hbm, w_hbm, ids_hbm, valid_hbm, tgt_hbm, p_ref, lp_ref,
                valid_ref, tgt_ref, ids_own, w, h, acc, ids_all, lane, tile, picks, packed, back, sbuf0, sbuf1,
                w_sem, own_sem, own_ids_sem, valid_sem, tgt_sem, h_recv, ids_recv, send_sem, back_send, back_recv):
    m = lax.axis_index('model')
    v = lax.axis_index('vocab')
    c = lax.rem(v, 2)
    me = m * 4 + v
    loc, width = h_hbm.shape
    shard_len = w_hbm.shape[0]
    list_len = ids_hbm.shape[1]
    quarter = width // 4
    half_w = width // 2
    rows_half = 8 * loc
    zp = m + 1 - 2 * lax.rem(m, 2)
    inner_n = m * (3 - m) // 2
    inner = inner_n == 1
    far_near = jnp.where(m < 2, 2, 1)
    far_far = jnp.where(m < 2, 3, 0)
    v_sib = v + 1 - 2 * c
    v_y = lax.rem(v + 2, 4)
    v_sy = lax.rem(v_sib + 2, 4)
    dev_y = {'vocab': v_y}
    dev_zp = {'model': zp}
    dev_sib = {'vocab': v_sib}
    dev_across = {'model': jnp.where(m < 2, 2, 1)}
    near_peers = (dev_y, dev_zp, dev_sib)

    n_chunks = pl.cdiv(shard_len, W_ROWS)

    def w_copy(i, half):
        n_rows = min(W_ROWS, shard_len - i * W_ROWS)
        at = (pl.ds(i * W_ROWS, n_rows), pl.ds(half * half_w, half_w))
        return pltpu.make_async_copy(w_hbm.at[at], w.at[at], w_sem.at[i, half])

    def row_block(blk):
        return pl.ds(pl.multiple_of(blk * loc, loc), loc)

    barrier = pltpu.get_barrier_semaphore()
    for d in near_peers:
        pl.semaphore_signal(barrier, inc=1, device_id=d, device_id_type=MESH)

    @pl.when(inner)
    def _():
        pl.semaphore_signal(barrier, inc=1, device_id=dev_across, device_id_type=MESH)

    own_h = pltpu.make_async_copy(h_hbm, h.at[row_block(me)], own_sem)
    own_h.start()
    own_valid = pltpu.make_async_copy(valid_hbm, valid_ref, valid_sem)
    own_tgt = pltpu.make_async_copy(tgt_hbm, tgt_ref, tgt_sem)
    own_ids = pltpu.make_async_copy(ids_hbm, ids_own, own_ids_sem)
    own_ids.start()
    own_valid.start()
    own_tgt.start()
    for half in range(2):
        for i in range(n_chunks):
            w_copy(i, half).start(priority=1)

    sent = {ALL: [], INNER: [], OUTER: []}

    def h_copy(k, blk, piece, dev):
        ref = h.at[row_block(blk), pl.ds(piece[0] * quarter, piece[1] * quarter)]
        return pltpu.make_async_remote_copy(ref, ref, send_sem.at[k], h_recv.at[blk, piece[0]],
                                            device_id=dev, device_id_type=MESH)

    def ids_copy(k, blk, dev):
        ref = ids_all.at[blk]
        return pltpu.make_async_remote_copy(ref, ref, send_sem.at[k], ids_recv.at[blk],
                                            device_id=dev, device_id_type=MESH)

    def start(make, who):
        i = len(sent[who])
        k = i if who == ALL else N_SENDS - 1 - i
        make(k).start()
        sent[who].append(functools.partial(make, k))

    def send_h(blk, piece, dev, who=0):
        start(lambda k: h_copy(k, blk, piece, dev), who)

    def send_ids(blk, dev, who=0):
        start(lambda k: ids_copy(k, blk, dev), who)

    def wait_h(blk, piece):
        h_copy(0, blk, piece, dev_sib).wait_recv()

    def wait_ids(blk):
        ids_copy(0, blk, dev_sib).wait_recv()

    def blk(zz, vv):
        return zz * 4 + vv

    b_y, b_z, b_d = blk(m, v_y), blk(zp, v), blk(zp, v_y)
    near_sib = (blk(m, v_sib), blk(m, v_sy), blk(zp, v_sib), blk(zp, v_sy))
    b_fn, b_ff, b_fny, b_ffy = blk(far_near, v), blk(far_far, v), blk(far_near, v_y), blk(far_far, v_y)
    far_sib = (blk(far_near, v_sib), blk(far_far, v_sib), blk(far_near, v_sy), blk(far_far, v_sy))
    quarters = tuple((q, 1) for q in range(4))
    halves = ((0, 2), (2, 2))

    own_ids.wait()
    ids_all[me] = jnp.concatenate([ids_own[: loc // 2, :], ids_own[loc // 2:, :]], axis=1)
    own_h.wait()
    pl.semaphore_wait(barrier, 3 + inner_n)

    send_h(me, quarters[0], dev_y)
    send_h(me, quarters[1], dev_zp)
    send_h(me, quarters[1], dev_y)
    send_h(me, quarters[0], dev_zp)

    @pl.when(inner)
    def _():
        send_h(me, halves[0], dev_across, INNER)

    send_h(me, halves[0], dev_sib)
    wait_h(b_y, quarters[0])
    send_h(b_y, quarters[0], dev_zp)
    wait_h(b_z, quarters[1])
    send_h(b_z, quarters[1], dev_y)
    send_h(me, quarters[2], dev_y)
    send_h(me, quarters[3], dev_zp)
    send_h(me, quarters[3], dev_y)
    send_h(me, quarters[2], dev_zp)
    send_h(me, halves[1], dev_sib)
    for d in near_peers:
        send_ids(me, d)
    wait_h(b_y, quarters[1])
    send_h(b_y, halves[0], dev_sib)
    wait_h(b_z, quarters[0])
    send_h(b_z, halves[0], dev_sib)

    @pl.when(inner)
    def _():
        send_h(b_z, halves[0], dev_across, INNER)
        send_h(me, halves[1], dev_across, INNER)
        send_ids(me, dev_across, INNER)

    def far(b, half):
        wait_h(b, halves[half])
        send_h(b, halves[half], dev_y, INNER)
        send_h(b, halves[half], dev_zp, INNER)
        send_h(b, halves[half], dev_sib, INNER)
        if half:
            wait_ids(b)
            for d in (dev_y, dev_zp, dev_sib):
                send_ids(b, d, INNER)

    def far_outer(b, half):
        wait_h(b, halves[half])
        send_h(b, halves[half], dev_y, OUTER)
        send_h(b, halves[half], dev_sib, OUTER)
        if half:
            wait_ids(b)
            for d in (dev_y, dev_sib):
                send_ids(b, d, OUTER)

    def far_y(b, half, who):
        wait_h(b, halves[half])
        send_h(b, halves[half], dev_sib, who)
        if half:
            wait_ids(b)
            send_ids(b, dev_sib, who)

    outer = inner_n == 0

    pl.when(inner)(lambda: far(b_fn, 0))
    wait_h(b_d, quarters[0])
    wait_h(b_d, quarters[1])
    send_h(b_d, halves[0], dev_sib)
    wait_h(b_y, quarters[2])
    send_h(b_y, quarters[2], dev_zp)
    wait_h(b_z, quarters[3])
    send_h(b_z, quarters[3], dev_y)
    for b in near_sib:
        wait_h(b, halves[0])

    def wait_w(half):
        for i in range(n_chunks):
            w_copy(i, half).wait()

    def a0_quarter():
        wait_h(b_y, quarters[3])
        send_h(b_y, halves[1], dev_sib)
        wait_h(b_z, quarters[2])
        send_h(b_z, halves[1], dev_sib)
        wait_ids(b_y)
        send_ids(b_y, dev_zp)
        send_ids(b_y, dev_sib)
        wait_ids(b_z)
        send_ids(b_z, dev_sib)

        @pl.when(inner)
        def _():
            send_h(b_z, halves[1], dev_across, INNER)
            send_ids(b_z, dev_across, INNER)
            far(b_ff, 0)

    def a0_half():
        @pl.when(inner)
        def _():
            far(b_fn, 1)
            far_y(b_fny, 0, INNER)

        pl.when(outer)(lambda: far_outer(b_fn, 0))

    def a0_three():
        wait_h(b_d, quarters[2])
        wait_h(b_d, quarters[3])
        send_h(b_d, halves[1], dev_sib)
        wait_ids(b_d)
        send_ids(b_d, dev_sib)

    def a1_start():
        @pl.when(inner)
        def _():
            far(b_ff, 1)
            far_y(b_ffy, 0, INNER)

        pl.when(outer)(lambda: far_outer(b_ff, 0))

    def a1_quarter():
        pl.when(inner)(lambda: far_y(b_fny, 1, INNER))

        @pl.when(outer)
        def _():
            far_outer(b_fn, 1)
            far_y(b_fny, 0, OUTER)

    def a1_three():
        pl.when(inner)(lambda: far_y(b_ffy, 1, INNER))

        @pl.when(outer)
        def _():
            far_outer(b_ff, 1)
            far_y(b_ffy, 0, OUTER)

    def b0_half():
        @pl.when(outer)
        def _():
            far_y(b_fny, 1, OUTER)
            far_y(b_ffy, 1, OUTER)

    picks[...] = jnp.zeros_like(picks)

    low = lax.broadcasted_iota(jnp.int32, (loc // 2, LANES), 1) < list_len

    def set_lists(b0):
        for i in range(8):
            off = ids_all[b0 + i] - me * shard_len
            turned = pltpu.roll(off, LANES - list_len, 1)
            for at, rows in ((0, jnp.where(low, off, turned)), (loc // 2, jnp.where(low, turned, off))):
                good = jnp.logical_and(rows >= 0, rows < shard_len)
                lane[i * loc + at:i * loc + at + loc // 2, :] = jnp.bitwise_and(rows, LANES - 1)
                tile[i * loc + at:i * loc + at + loc // 2, :] = jnp.where(good, lax.shift_right_arithmetic(rows, 7), 1 << 20)

    sbufs = (sbuf0, sbuf1)
    n_pairs = w.shape[0] // PAIR

    def run_pass(r0, half, points):
        hr = pl.ds(r0, rows_half)
        kc = pl.ds(half * half_w, half_w)

        def pick(s_ref, t0):
            for q in range(PAIR // LANES):
                g = jnp.take_along_axis(s_ref[:, q * LANES:(q + 1) * LANES], lane[...], axis=1)
                picks[hr, :] = jnp.where(tile[...] == t0 + q, g, picks[hr, :])

        for j in range(n_pairs):
            if j in points:
                points[j]()
            prod = lax.dot_general(h[hr, kc], w[pl.ds(j * PAIR, PAIR), kc], (((1,), (1,)), ((), ())),
                                   preferred_element_type=jnp.float32)
            if half == 0:
                acc[j] = prod
            else:
                sbufs[j % 2][...] = prod + acc[j]
                if j:
                    pick(sbufs[(j + 1) % 2], (j - 1) * (PAIR // LANES))
        if half:
            pick(sbufs[(n_pairs - 1) % 2], (n_pairs - 1) * (PAIR // LANES))


    def pack(r0, p0):
        for i in range(8):
            top = picks[pl.ds(pl.multiple_of(r0 + i * loc, loc // 2), loc // 2), :]
            bot = picks[pl.ds(pl.multiple_of(r0 + i * loc + loc // 2, loc // 2), loc // 2), :]
            packed[p0 + i] = jnp.where(low, top, bot)

    def send_back(zz, vv, i):
        cp = pltpu.make_async_remote_copy(packed.at[blk(zz, vv)], back.at[me], back_send.at[i], back_recv.at[me],
                                          device_id={'model': zz, 'vocab': vv}, device_id_type=MESH)
        cp.start()
        return cp

    r_a = pl.multiple_of((m // 2) * rows_half, rows_half)
    r_b = pl.multiple_of((1 - m // 2) * rows_half, rows_half)
    own_valid.wait()
    own_tgt.wait()
    wait_w(0)
    run_pass(r_a, 0, {4: a0_quarter, 8: a0_half, 12: a0_three})
    for b in near_sib:
        wait_ids(b)
        wait_h(b, halves[1])
    a1_start()
    set_lists((m // 2) * 8)
    wait_w(1)
    run_pass(r_a, 1, {4: a1_quarter, 12: a1_three})
    pack(r_a, (m // 2) * 8)
    backs = []
    for i, (zz, dv) in enumerate([(zp, 2), (zp, 3), (zp, 0), (zp, 1), (m, 2), (m, 1), (m, 3)]):
        backs.append(send_back(zz, lax.rem(v + dv, 4), i))
    for b in far_sib:
        wait_h(b, halves[0])
    run_pass(r_b, 0, {8: b0_half})
    for b in far_sib:
        wait_ids(b)
        wait_h(b, halves[1])
    set_lists((1 - m // 2) * 8)
    run_pass(r_b, 1, {})
    pack(r_b, (1 - m // 2) * 8)
    for i, (zz, dv) in enumerate([(zf, dv) for zf in (far_far, far_near) for dv in (2, 3, 0, 1)]):
        backs.append(send_back(zz, lax.rem(v + dv, 4), 7 + i))

    back[me] = packed[me]
    total = back[me]
    for dz in range(4):
        for dv in range(4):
            if dz == 0 and dv == 0:
                continue
            b = blk(lax.rem(m + dz, 4), lax.rem(v + dv, 4))
            pltpu.make_async_remote_copy(back.at[b], back.at[b], back_send.at[0], back_recv.at[b],
                                         device_id=dev_sib, device_id_type=MESH).wait_recv()
            total = total + back[b]
    total = jnp.concatenate([total, pltpu.roll(total, LANES - list_len, 1)], axis=0)[:, :list_len]
    is_valid = valid_ref[...] > 0
    scores = jnp.where(is_valid, total / TEMPERATURE, -jnp.inf)
    top = jnp.max(scores, axis=1, keepdims=True)
    log_norm = top + jnp.log(jnp.sum(jnp.exp(scores - top), axis=1, keepdims=True))
    p_ref[...] = jnp.where(is_valid, jnp.exp(scores - log_norm), 0.0)
    eye = lax.broadcasted_iota(jnp.int32, (loc, loc), 0) == lax.broadcasted_iota(jnp.int32, (loc, loc), 1)
    tgt_col = jnp.sum(jnp.where(eye, tgt_ref[...], 0), axis=1, keepdims=True)
    hit = lax.broadcasted_iota(jnp.int32, (loc, list_len), 1) == tgt_col
    picked = jnp.sum(jnp.where(hit, scores, 0.0), axis=1, keepdims=True)
    lp_ref[...] = jnp.sum(jnp.where(eye, picked - log_norm, 0.0), axis=0, keepdims=True)
    assert len(sent[ALL]) + max(len(sent[INNER]), len(sent[OUTER])) == N_SENDS
    for make in sent[ALL]:
        make().wait_send()

    @pl.when(inner)
    def _():
        for make in sent[INNER]:
            make().wait_send()

    @pl.when(outer)
    def _():
        for make in sent[OUTER]:
            make().wait_send()

    for cp in backs:
        cp.wait_send()


def solution(mesh):
    axes = ('model', 'vocab')
    row_spec = P(('rep',) + axes, None)
    vec_spec = P(('rep',) + axes)

    def local_step(hidden, head_rows, allowed_ids, valid_mask, target_pos):
        loc, width = hidden.shape
        list_len = allowed_ids.shape[1]
        rows = 16 * loc
        w_rows = pl.cdiv(head_rows.shape[0], PAIR) * PAIR
        any_spec = pl.BlockSpec(memory_space=pl.ANY)
        vmem = pl.BlockSpec(memory_space=pltpu.VMEM)
        dma = pltpu.SemaphoreType.DMA
        p, lp = pl.pallas_call(
            head_kernel,
            out_shape=(pltpu.VMEM((loc, list_len), jnp.float32), pltpu.VMEM((1, loc), jnp.float32)),
            in_specs=[any_spec] * 5,
            out_specs=(vmem, vmem),
            scratch_shapes=[
                pltpu.VMEM((loc, list_len), jnp.int32),
                pltpu.VMEM((1, loc), jnp.int32),
                pltpu.VMEM((loc, list_len), jnp.int32),
                pltpu.VMEM((w_rows, width), jnp.bfloat16),
                pltpu.VMEM((rows, width), jnp.bfloat16),
                pltpu.VMEM((w_rows // PAIR, rows // 2, PAIR), jnp.float32),
                pltpu.VMEM((16, loc // 2, LANES), jnp.int32),
                pltpu.VMEM((rows // 2, LANES), jnp.int32),
                pltpu.VMEM((rows // 2, LANES), jnp.int32),
                pltpu.VMEM((rows, LANES), jnp.float32),
                pltpu.VMEM((16, loc // 2, LANES), jnp.float32),
                pltpu.VMEM((16, loc // 2, LANES), jnp.float32),
                pltpu.VMEM((rows // 2, PAIR), jnp.float32),
                pltpu.VMEM((rows // 2, PAIR), jnp.float32),
                dma((pl.cdiv(head_rows.shape[0], W_ROWS), 2)),
                dma, dma, dma, dma,
                dma((16, 4)),
                dma((16,)),
                dma((N_SENDS,)),
                dma((16,)),
                dma((16,)),
            ],
            compiler_params=pltpu.CompilerParams(collective_id=0, has_side_effects=True, vmem_limit_bytes=65500000),
        )(hidden, head_rows, allowed_ids, valid_mask, target_pos.reshape(1, loc))
        return p, lp.reshape(loc)

    return jax.shard_map(local_step, mesh=mesh, in_specs=(row_spec, P(axes, None), row_spec, row_spec, vec_spec),
                         out_specs=(row_spec, vec_spec), check_vma=False)
```
